32 devices in a mesh: gx: 4 (over y, x), gy: 2 (over core), gz: 4 (over z).
Axes of the slice: x: 2, y: 2, z: 4, core: 2. Of those that a mesh axis runs over, the one named last changes fastest.
Arguments:
- measures: float32 [65536, 256], P(('gx', 'gy', 'gz')), may hold values from -6 to 6
- group_index: int32 [65536], P(('gx', 'gy', 'gz')), may hold values from 0 to 511, as said below
- distinct_keys: int32 [32, 512], P(('gx', 'gy', 'gz')), may hold values from 32 to 65567, as said below
- group_counts: int32 [32], P(('gx', 'gy', 'gz')), may hold values from 128 to 512, as said below
Outputs:
- group_sums: float32 [16384, 256], P(('gx', 'gy', 'gz'))
- group_rows: int32 [16384], P(('gx', 'gy', 'gz'))
- group_keys: int32 [16384], P(('gx', 'gy', 'gz'))
- group_total: int32 [], replicated
The draws below stay inside these ranges and needn't reach their ends.
Inputs may be any that keep to these rules, and one draw needn't show every extreme that they name: `group_counts`: every device has between 128 and 512 groups, and some device has exactly 512. `group_index`: each row's index lies below its device's group count, and every group of a device has at least one row. `distinct_keys`: each device's keys rise strictly; all keys of device d equal d modulo 32, so no key lives on two devices; entries at and past the device's count are unused.
All inputs are finite; a program needn't handle non-finite values.
Results may differ from the reference program's by a relative error of at most 0.0003.
Values sent between devices are 32-bit elements; how exact they have to be, the bound alone decides.
No kernel may reach another device: no remote copies, remote signals or barrier semaphores. Data moves between devices by JAX's collectives and lax.ppermute only.
A program may use at most 64 MiB of HBM per device.

```python
import jax
import jax.numpy as jnp
from jax import lax

ROW_DEV = 2048
M = 256
GMAX = 512
ROWS = 65536
DEVICES = 32


def shared_counts(key):
    counts = jax.random.randint(jax.random.fold_in(key, 7), (DEVICES,), GMAX // 4, GMAX + 1)
    fullest = jax.random.randint(jax.random.fold_in(key, 8), (), 0, DEVICES)
    return counts.at[fullest].set(GMAX).astype(jnp.int32)


def draw_group_counts(key, part):
    return shared_counts(key)


def one_device(key, count):
    places = jnp.arange(ROW_DEV, dtype=jnp.int32)
    upper = jnp.minimum(jax.random.randint(jax.random.fold_in(key, 1), (ROW_DEV,), 1, GMAX + 1), count)
    picked = jax.random.randint(jax.random.fold_in(key, 2), (ROW_DEV,), 0, upper)
    picked = jnp.where(places < count, places, picked % count)
    order = jax.random.permutation(jax.random.fold_in(key, 3), ROW_DEV)
    return picked[order].astype(jnp.int32)


def draw_group_index(key, part):
    counts = shared_counts(key)
    device_keys = jax.vmap(lambda d: jax.random.fold_in(jax.random.fold_in(key, 11), d))(jnp.arange(DEVICES))
    return jax.vmap(one_device)(device_keys, counts).reshape(-1)


def draw_distinct_keys(key, part):
    steps = jax.random.randint(jax.random.fold_in(key, 21), (DEVICES, GMAX), 1, 5)
    steps = steps.at[0, 0].set(1)
    rising = jnp.cumsum(steps, axis=1)
    rising = rising.at[:, GMAX - 1].set(4 * GMAX)
    owner = jnp.arange(DEVICES, dtype=jnp.int32)[:, None]
    return (owner + DEVICES * rising).astype(jnp.int32)


def shard_levels(key, extent, pieces, least, top_value):
    loudness = 1.0
    for dim, blocks in pieces:
        draws = jax.random.uniform(jax.random.fold_in(jax.random.fold_in(key, 6), dim), (blocks,), jnp.float32, least / len(pieces), top_value / len(pieces))
        loudness = loudness * jnp.repeat(jnp.exp(draws), extent[dim] // blocks).reshape((-1,) + (1,) * (len(extent) - 1 - dim))
    return loudness


def gaussian(key, dims, width, limit, split=(), held_as=jnp.bfloat16):
    drawn = width * jax.random.normal(key, dims, jnp.float32)
    if split:
        drawn = drawn * shard_levels(key, dims, split, -0.22, 0.18)
    return jnp.clip(drawn, -limit, limit).astype(held_as)


def setup_inputs(seed: int = 0) -> dict:
    arg_keys = jax.random.split(jax.random.key(seed), 5)
    measures = gaussian(arg_keys[0], (ROWS, M), 1.0, 6.0, ((0, 32),), jnp.float32)
    group_index = draw_group_index(jax.random.fold_in(arg_keys[4], 71), 0)
    distinct_keys = draw_distinct_keys(jax.random.fold_in(arg_keys[4], 71), 0)
    group_counts = draw_group_counts(jax.random.fold_in(arg_keys[4], 71), 0)
    return dict(measures=measures, group_index=group_index, distinct_keys=distinct_keys, group_counts=group_counts)


def local_groups(pair):
    values, index = pair
    sums = jax.ops.segment_sum(values, index, num_segments=GMAX)
    rows = jax.ops.segment_sum(jnp.ones_like(index), index, num_segments=GMAX)
    return sums, rows


def reference(measures, group_index, distinct_keys, group_counts):
    offsets = jnp.cumsum(group_counts) - group_counts
    group_total = jnp.sum(group_counts).astype(jnp.int32)
    values = measures.reshape(DEVICES, ROW_DEV, M)
    index = group_index.reshape(DEVICES, ROW_DEV)
    sums, rows = lax.map(local_groups, (values, index))
    local = jnp.arange(GMAX, dtype=jnp.int32)
    dense = offsets[:, None] + local[None, :]
    live = local[None, :] < group_counts[:, None]
    where_to = (dense % DEVICES) * GMAX + dense // DEVICES
    where_to = jnp.where(live, where_to, DEVICES * GMAX).astype(jnp.int32).reshape(-1)
    group_sums = jnp.zeros((DEVICES * GMAX, M), jnp.float32).at[where_to].set(sums.reshape(-1, M), mode="drop")
    group_rows = jnp.zeros((DEVICES * GMAX,), jnp.int32).at[where_to].set(rows.reshape(-1).astype(jnp.int32), mode="drop")
    group_keys = jnp.full((DEVICES * GMAX,), -1, jnp.int32).at[where_to].set(distinct_keys.reshape(-1), mode="drop")
    return group_sums, group_rows, group_keys, group_total
```

```python
import functools

import jax
import jax.numpy as jnp
from jax import lax
from jax.experimental import pallas as pl
from jax.experimental.pallas import tpu as pltpu
from jax.sharding import PartitionSpec as P

AXES = ("gx", "gy", "gz")
LANES = 128


def split3(x):
    high = x.astype(jnp.bfloat16)
    rest = x - high.astype(jnp.float32)
    middle = rest.astype(jnp.bfloat16)
    low = (rest - middle.astype(jnp.float32)).astype(jnp.bfloat16)
    return high, middle, low


def local_kernel(devices, slots, index_ref, values_ref, keys_ref, packed_ref, sums_ref, fields_ref):
    step = pl.program_id(0)
    span, width = sums_ref.shape
    rows = values_ref.shape[0]
    parts = width // LANES
    each = slots * parts + 1

    @pl.when(step == 0)
    def _():
        sums_ref[...] = jnp.zeros_like(sums_ref)
        fields_ref[...] = keys_ref[...]

    index = index_ref[...]
    residue = index % devices
    level = index // devices
    place = residue * slots + level
    hits = (place == lax.broadcasted_iota(jnp.int32, (span, rows), 0)).astype(jnp.bfloat16)
    total = sums_ref[...]
    for part in split3(values_ref[...]):
        total = total + jnp.dot(hits, part, preferred_element_type=jnp.float32)
    sums_ref[...] = total
    by_residue = (residue == lax.broadcasted_iota(jnp.int32, (devices, rows), 0)).astype(jnp.bfloat16)
    by_level = (level == lax.broadcasted_iota(jnp.int32, (LANES, rows), 0)).astype(jnp.bfloat16)
    fields_ref[...] += lax.dot_general(
        by_residue, by_level, (((1,), (1,)), ((), ())), preferred_element_type=jnp.float32
    )

    @pl.when(step == pl.num_programs(0) - 1)
    def _():
        for device in range(devices):
            for copy in (device, device + devices):
                start = copy * each
                for part in range(parts):
                    packed_ref[start + part * slots : start + (part + 1) * slots, :] = sums_ref[
                        device * slots : (device + 1) * slots, part * LANES : (part + 1) * LANES
                    ]
                packed_ref[start + each - 1 : start + each, :] = fields_ref[device : device + 1, :]


def place_kernel(devices, slots, counts_ref, me_ref, got_ref, sums_ref, rows_ref, keys_ref, room_ref, mask_ref):
    span, width = sums_ref.shape
    parts = width // LANES
    each = slots * parts + 1
    me = me_ref[0]
    room_ref[...] = jnp.zeros_like(room_ref)
    window = room_ref.shape[0] - span
    spot = lax.broadcasted_iota(jnp.int32, (1, span), 1)
    line = lax.broadcasted_iota(jnp.int32, (window, width), 0)
    padding = jnp.zeros((window - slots, width), jnp.float32)
    offset = jnp.int32(0)
    end = jnp.int32(0)
    level = jnp.zeros((1, span), jnp.int32)
    for sender in range(devices):
        base = end
        offset = offset + counts_ref[sender]
        end = lax.div(offset - me + (devices - 1), devices)
        first = sender * each
        chunk = jnp.concatenate(
            [got_ref[first + part * slots : first + (part + 1) * slots, :] for part in range(parts)], axis=1
        )
        shift = base % 8
        chunk = pltpu.roll(jnp.concatenate([chunk, padding], axis=0), shift, 0)
        there = pl.ds(pl.multiple_of(base - shift, 8), window)
        room_ref[there, :] = jnp.where((line >= shift) & (line < shift + end - base), chunk, room_ref[there, :])
        inside = (spot >= base) & (spot < end)
        mask_ref[sender : sender + 1, :] = inside.astype(jnp.float32)
        level = jnp.where(inside, spot - base, level)
    sums_ref[...] = room_ref[:span, :]
    fields = jnp.concatenate(
        [got_ref[(sender + 1) * each - 1 : (sender + 1) * each, :] for sender in range(devices)], axis=0
    )
    picked = lax.dot_general(
        fields,
        mask_ref[...],
        (((0,), (0,)), ((), ())),
        precision=lax.Precision.HIGHEST,
        preferred_element_type=jnp.float32,
    )
    field = lax.broadcasted_iota(jnp.int32, (LANES, span), 0)
    rows = jnp.sum(jnp.where(field == level, picked, 0.0), axis=0, keepdims=True)
    keys = jnp.sum(jnp.where(field == level + slots, picked, 0.0), axis=0, keepdims=True)
    live = spot < end
    rows = jnp.where(live, rows, 0.0).astype(jnp.int32)
    keys = jnp.where(live, keys, -1.0).astype(jnp.int32)
    for part in range(span // LANES):
        rows_ref[part : part + 1, :] = rows[:, part * LANES : (part + 1) * LANES]
        keys_ref[part : part + 1, :] = keys[:, part * LANES : (part + 1) * LANES]


def shards(measures, group_index, distinct_keys, group_counts):
    rows, width = measures.shape
    span = distinct_keys.shape[1]
    devices = lax.axis_size(AXES)
    slots = span // devices
    parts = width // LANES
    each = slots * parts + 1
    me = lax.axis_index(AXES)
    counts = lax.all_to_all(
        jnp.broadcast_to(group_counts.reshape(1, 1, 1), (devices, 1, LANES)), AXES, split_axis=0, concat_axis=0, tiled=True
    )[:, 0, 0]
    keys = distinct_keys[0].reshape(slots, devices).T.astype(jnp.float32)
    keys = jnp.pad(keys, ((0, 0), (slots, LANES - 2 * slots)))
    block = min(512, rows)
    packed = pl.pallas_call(
        functools.partial(local_kernel, devices, slots),
        grid=(rows // block,),
        in_specs=[
            pl.BlockSpec((1, block), lambda i: (0, i)),
            pl.BlockSpec((block, width), lambda i: (i, 0)),
            pl.BlockSpec((devices, LANES), lambda i: (0, 0)),
        ],
        out_specs=pl.BlockSpec((2 * devices * each, LANES), lambda i: (0, 0)),
        out_shape=jax.ShapeDtypeStruct((2 * devices * each, LANES), jnp.float32),
        scratch_shapes=[pltpu.VMEM((span, width), jnp.float32), pltpu.VMEM((devices, LANES), jnp.float32)],
        cost_estimate=pl.CostEstimate(flops=6 * span * rows * width, bytes_accessed=4 * rows * width, transcendentals=0),
        name="local",
    )(group_index.reshape(1, rows), measures, keys)
    ahead = jnp.arange(devices, dtype=jnp.int32) < me
    offset = jnp.sum(jnp.where(ahead, counts, 0)) % devices
    outgoing = lax.dynamic_slice_in_dim(packed.reshape(2 * devices, 1, each * LANES), devices - offset, devices, 0)
    got = lax.all_to_all(outgoing, AXES, split_axis=0, concat_axis=0, tiled=True)
    group_total = jnp.sum(counts)
    group_sums, group_rows, group_keys = pl.pallas_call(
        functools.partial(place_kernel, devices, slots),
        in_specs=[
            pl.BlockSpec(memory_space=pltpu.SMEM),
            pl.BlockSpec(memory_space=pltpu.SMEM),
            pl.BlockSpec(memory_space=pltpu.VMEM),
        ],
        out_specs=[pl.BlockSpec(memory_space=pltpu.VMEM)] * 3,
        out_shape=[
            jax.ShapeDtypeStruct((span, width), jnp.float32),
            jax.ShapeDtypeStruct((span // LANES, LANES), jnp.int32),
            jax.ShapeDtypeStruct((span // LANES, LANES), jnp.int32),
        ],
        scratch_shapes=[pltpu.VMEM((span + -(-slots // 8) * 8 + 8, width), jnp.float32), pltpu.VMEM((devices, span), jnp.float32)],
        name="place",
    )(counts, me.reshape(1), got.reshape(devices * each, LANES))
    return group_sums, group_rows.reshape(span), group_keys.reshape(span), group_total


def solution(mesh):
    return jax.shard_map(
        shards,
        mesh=mesh,
        in_specs=(P(AXES, None), P(AXES), P(AXES, None), P(AXES)),
        out_specs=(P(AXES, None), P(AXES), P(AXES), P()),
        check_vma=False,
    )
```

```python
import functools

import jax
import jax.numpy as jnp
from jax import lax
from jax.experimental import pallas as pl
from jax.experimental.pallas import tpu as pltpu
from jax.sharding import PartitionSpec as P

AXES = ("gx", "gy", "gz")
LANES = 128


def split3(x):
    high = x.astype(jnp.bfloat16)
    rest = x - high.astype(jnp.float32)
    middle = rest.astype(jnp.bfloat16)
    low = (rest - middle.astype(jnp.float32)).astype(jnp.bfloat16)
    return high, middle, low


def local_kernel(devices, slots, index_ref, values_ref, keys_ref, packed_ref, sums_ref, fields_ref):
    step = pl.program_id(0)
    span, width = sums_ref.shape
    rows = values_ref.shape[0]
    parts = width // LANES
    each = slots * parts + 1

    @pl.when(step == 0)
    def _():
        sums_ref[...] = jnp.zeros_like(sums_ref)
        fields_ref[...] = keys_ref[...]

    index = index_ref[...]
    residue = index % devices
    level = index // devices
    place = residue * slots + level
    hits = (place == lax.broadcasted_iota(jnp.int32, (span, rows), 0)).astype(jnp.bfloat16)
    total = sums_ref[...]
    for part in split3(values_ref[...]):
        total = total + jnp.dot(hits, part, preferred_element_type=jnp.float32)
    sums_ref[...] = total
    by_residue = (residue == lax.broadcasted_iota(jnp.int32, (devices, rows), 0)).astype(jnp.bfloat16)
    by_level = (level == lax.broadcasted_iota(jnp.int32, (LANES, rows), 0)).astype(jnp.bfloat16)
    fields_ref[...] += lax.dot_general(
        by_residue, by_level, (((1,), (1,)), ((), ())), preferred_element_type=jnp.float32
    )

    @pl.when(step == pl.num_programs(0) - 1)
    def _():
        for device in range(devices):
            for copy in (device, device + devices):
                start = copy * each
                for part in range(parts):
                    packed_ref[start + part * slots : start + (part + 1) * slots, :] = sums_ref[
                        device * slots : (device + 1) * slots, part * LANES : (part + 1) * LANES
                    ]
                packed_ref[start + each - 1 : start + each, :] = fields_ref[device : device + 1, :]


def spread_kernel(count_ref, out_ref):
    out_ref[...] = jnp.full(out_ref.shape, count_ref[0], jnp.int32)


def roll_kernel(devices, pieces, me_ref, counts_ref, packed_ref, out_ref, room_ref, in_sem, out_sem):
    counts = counts_ref[...].astype(jnp.float32)
    sender = lax.broadcasted_iota(jnp.int32, counts.shape, 0)
    lane = lax.broadcasted_iota(jnp.int32, counts.shape, 1)
    offset = jnp.sum(jnp.where((sender < me_ref[0]) & (lane == 0), counts, 0.0)).astype(jnp.int32)
    start = devices - lax.rem(offset, devices)
    each = devices // pieces
    into = [
        pltpu.make_async_copy(
            packed_ref.at[pl.ds(start + piece * each, each)], room_ref.at[pl.ds(piece * each, each)], in_sem.at[piece]
        )
        for piece in range(pieces)
    ]
    out = [
        pltpu.make_async_copy(
            room_ref.at[pl.ds(piece * each, each)], out_ref.at[pl.ds(piece * each, each)], out_sem.at[piece]
        )
        for piece in range(pieces)
    ]
    for copy in into:
        copy.start()
    for piece in range(pieces):
        into[piece].wait()
        out[piece].start()
    for copy in out:
        copy.wait()


def place_kernel(
    devices, slots, pieces, me_ref, held_ref, all_ref, sums_ref, rows_ref, keys_ref, total_ref,
    counts_ref, got_ref, room_ref, mask_ref, counts_sem, sem
):
    span, width = sums_ref.shape
    parts = width // LANES
    each = slots * parts + 1
    me = me_ref[0]
    group = devices // pieces
    copies = [
        pltpu.make_async_copy(
            all_ref.at[pl.ds(piece * group * each, group * each)],
            got_ref.at[pl.ds(piece * group * each, group * each)],
            sem.at[piece],
        )
        for piece in range(pieces)
    ]
    counts_copy = pltpu.make_async_copy(held_ref, counts_ref, counts_sem)
    counts_copy.start()
    for copy in copies:
        copy.start()
    room_ref[...] = jnp.zeros_like(room_ref)
    window = room_ref.shape[0] - span
    spot = lax.broadcasted_iota(jnp.int32, (1, span), 1)
    line = lax.broadcasted_iota(jnp.int32, (window, width), 0)
    padding = jnp.zeros((window - slots, width), jnp.float32)
    counts_copy.wait()
    offset = jnp.int32(0)
    end = jnp.int32(0)
    level = jnp.zeros((1, span), jnp.int32)
    for sender in range(devices):
        if sender % group == 0:
            copies[sender // group].wait()
        base = end
        offset = offset + counts_ref[sender, 0]
        end = lax.div(offset - me + (devices - 1), devices)
        first = sender * each
        chunk = jnp.concatenate(
            [got_ref[first + part * slots : first + (part + 1) * slots, :] for part in range(parts)], axis=1
        )
        shift = base % 8
        chunk = pltpu.roll(jnp.concatenate([chunk, padding], axis=0), shift, 0)
        there = pl.ds(pl.multiple_of(base - shift, 8), window)
        room_ref[there, :] = jnp.where((line >= shift) & (line < shift + end - base), chunk, room_ref[there, :])
        inside = (spot >= base) & (spot < end)
        mask_ref[sender : sender + 1, :] = inside.astype(jnp.float32)
        level = jnp.where(inside, spot - base, level)
    sums_ref[...] = room_ref[:span, :]
    total_ref[0] = offset
    fields = jnp.concatenate(
        [got_ref[(sender + 1) * each - 1 : (sender + 1) * each, :] for sender in range(devices)], axis=0
    )
    picked = lax.dot_general(
        fields,
        mask_ref[...],
        (((0,), (0,)), ((), ())),
        precision=lax.Precision.HIGHEST,
        preferred_element_type=jnp.float32,
    )
    field = lax.broadcasted_iota(jnp.int32, (LANES, span), 0)
    rows = jnp.sum(jnp.where(field == level, picked, 0.0), axis=0, keepdims=True)
    keys = jnp.sum(jnp.where(field == level + slots, picked, 0.0), axis=0, keepdims=True)
    live = spot < end
    rows = jnp.where(live, rows, 0.0).astype(jnp.int32)
    keys = jnp.where(live, keys, -1.0).astype(jnp.int32)
    for part in range(span // LANES):
        rows_ref[part : part + 1, :] = rows[:, part * LANES : (part + 1) * LANES]
        keys_ref[part : part + 1, :] = keys[:, part * LANES : (part + 1) * LANES]


def shards(measures, group_index, distinct_keys, group_counts):
    rows, width = measures.shape
    span = distinct_keys.shape[1]
    devices = lax.axis_size(AXES)
    slots = span // devices
    parts = width // LANES
    each = slots * parts + 1
    me = lax.axis_index(AXES)
    pieces = 4
    spread = pl.pallas_call(
        spread_kernel,
        in_specs=[pl.BlockSpec(memory_space=pltpu.SMEM)],
        out_specs=pl.BlockSpec(memory_space=pltpu.VMEM),
        out_shape=jax.ShapeDtypeStruct((devices, LANES), jnp.int32),
        name="spread",
    )(group_counts)
    counts = lax.all_to_all(spread.reshape(devices, 1, LANES), AXES, split_axis=0, concat_axis=0, tiled=True)
    counts = counts.reshape(devices, LANES)
    keys = distinct_keys[0].reshape(slots, devices).T.astype(jnp.float32)
    keys = jnp.pad(keys, ((0, 0), (slots, LANES - 2 * slots)))
    block = min(512, rows)
    packed = pl.pallas_call(
        functools.partial(local_kernel, devices, slots),
        grid=(rows // block,),
        in_specs=[
            pl.BlockSpec((1, block), lambda i: (0, i)),
            pl.BlockSpec((block, width), lambda i: (i, 0)),
            pl.BlockSpec((devices, LANES), lambda i: (0, 0)),
        ],
        out_specs=pl.BlockSpec((2 * devices * each, LANES), lambda i: (0, 0)),
        out_shape=jax.ShapeDtypeStruct((2 * devices * each, LANES), jnp.float32),
        scratch_shapes=[pltpu.VMEM((span, width), jnp.float32), pltpu.VMEM((devices, LANES), jnp.float32)],
        cost_estimate=pl.CostEstimate(flops=6 * span * rows * width, bytes_accessed=4 * rows * width, transcendentals=0),
        name="local",
    )(group_index.reshape(1, rows), measures, keys)
    outgoing = pl.pallas_call(
        functools.partial(roll_kernel, devices, pieces),
        in_specs=[
            pl.BlockSpec(memory_space=pltpu.SMEM),
            pl.BlockSpec(memory_space=pltpu.VMEM),
            pl.BlockSpec(memory_space=pl.ANY),
        ],
        out_specs=pl.BlockSpec(memory_space=pl.ANY),
        out_shape=jax.ShapeDtypeStruct((devices, 1, each * LANES), jnp.float32),
        scratch_shapes=[
            pltpu.VMEM((devices, 1, each * LANES), jnp.float32),
            pltpu.SemaphoreType.DMA((pieces,)),
            pltpu.SemaphoreType.DMA((pieces,)),
        ],
        name="roll",
    )(me.reshape(1), counts, packed.reshape(2 * devices, 1, each * LANES))
    got = lax.all_to_all(outgoing, AXES, split_axis=0, concat_axis=0, tiled=True)
    group_sums, group_rows, group_keys, group_total = pl.pallas_call(
        functools.partial(place_kernel, devices, slots, pieces),
        in_specs=[
            pl.BlockSpec(memory_space=pltpu.SMEM),
            pl.BlockSpec(memory_space=pltpu.VMEM),
            pl.BlockSpec(memory_space=pl.ANY),
        ],
        out_specs=[pl.BlockSpec(memory_space=pltpu.VMEM)] * 3 + [pl.BlockSpec(memory_space=pltpu.SMEM)],
        out_shape=[
            jax.ShapeDtypeStruct((span, width), jnp.float32),
            jax.ShapeDtypeStruct((span // LANES, LANES), jnp.int32),
            jax.ShapeDtypeStruct((span // LANES, LANES), jnp.int32),
            jax.ShapeDtypeStruct((1,), jnp.int32),
        ],
        scratch_shapes=[
            pltpu.SMEM((devices, LANES), jnp.int32),
            pltpu.VMEM((devices * each, LANES), jnp.float32),
            pltpu.VMEM((span + -(-slots // 8) * 8 + 8, width), jnp.float32),
            pltpu.VMEM((devices, span), jnp.float32),
            pltpu.SemaphoreType.DMA,
            pltpu.SemaphoreType.DMA((pieces,)),
        ],
        name="place",
    )(me.reshape(1), counts, got.reshape(devices * each, LANES))
    return group_sums, group_rows.reshape(span), group_keys.reshape(span), group_total.reshape(())


def solution(mesh):
    return jax.shard_map(
        shards,
        mesh=mesh,
        in_specs=(P(AXES, None), P(AXES), P(AXES, None), P(AXES)),
        out_specs=(P(AXES, None), P(AXES), P(AXES), P()),
        check_vma=False,
    )
```

```python
import functools

import jax
import jax.numpy as jnp
from jax import lax
from jax.experimental import pallas as pl
from jax.experimental.pallas import tpu as pltpu
from jax.sharding import PartitionSpec as P

AXES = ("gx", "gy", "gz")
LANES = 128
MIB = 1024 * 1024


def split3(x):
    high = x.astype(jnp.bfloat16)
    rest = x - high.astype(jnp.float32)
    middle = rest.astype(jnp.bfloat16)
    low = (rest - middle.astype(jnp.float32)).astype(jnp.bfloat16)
    return high, middle, low


def local_kernel(devices, slots, block, index_ref, values_ref, keys_ref, packed_ref, sums_ref, fields_ref):
    span, width = sums_ref.shape
    rows = values_ref.shape[0]
    parts = width // LANES
    each = slots * parts + 1

    def one_hot(height, place):
        return place == lax.broadcasted_iota(jnp.int32, (height, place.shape[1]), 0)

    def across(left, right):
        return lax.dot_general(left, right, (((1,), (1,)), ((), ())), preferred_element_type=jnp.float32)

    group = lax.broadcasted_iota(jnp.int32, (1, span), 1)
    to_residue = one_hot(devices, group % devices).astype(jnp.bfloat16)
    to_level = jnp.where(one_hot(LANES, group // devices + slots), keys_ref[...].astype(jnp.float32), 0.0)
    fields = jnp.zeros(fields_ref.shape, jnp.float32)
    for part in split3(to_level):
        fields = fields + across(to_residue, part)
    for start in range(0, rows, block):
        index = index_ref[:, start : start + block]
        residue = index % devices
        level = index // devices
        hits = one_hot(span, residue * slots + level).astype(jnp.bfloat16)
        high, middle, low = split3(values_ref[start : start + block, :])
        total = jnp.dot(hits, high, preferred_element_type=jnp.float32)
        total = total + jnp.dot(hits, middle, preferred_element_type=jnp.float32)
        total = total + jnp.dot(hits, low, preferred_element_type=jnp.float32)
        sums_ref[...] = total if start == 0 else sums_ref[...] + total
        fields = fields + across(
            one_hot(devices, residue).astype(jnp.bfloat16), one_hot(LANES, level).astype(jnp.bfloat16)
        )
    fields_ref[...] = fields
    for device in range(devices):
        for copy in (device, device + devices):
            start = copy * each
            for part in range(parts):
                packed_ref[start + part * slots : start + (part + 1) * slots, :] = sums_ref[
                    device * slots : (device + 1) * slots, part * LANES : (part + 1) * LANES
                ]
            packed_ref[start + each - 1 : start + each, :] = fields_ref[device : device + 1, :]


def spread_kernel(count_ref, out_ref):
    out_ref[...] = jnp.full(out_ref.shape, count_ref[0], jnp.int32)


def roll_kernel(devices, me_ref, counts_ref, packed_ref, out_ref, sem):
    counts = counts_ref[...].astype(jnp.float32)
    sender = lax.broadcasted_iota(jnp.int32, counts.shape, 0)
    lane = lax.broadcasted_iota(jnp.int32, counts.shape, 1)
    offset = jnp.sum(jnp.where((sender < me_ref[0]) & (lane == 0), counts, 0.0)).astype(jnp.int32)
    start = devices - lax.rem(offset, devices)
    copy = pltpu.make_async_copy(packed_ref.at[pl.ds(start, devices)], out_ref, sem)
    copy.start()
    copy.wait()


def place_kernel(
    devices, slots, me_ref, held_ref, got_ref, sums_ref, rows_ref, keys_ref, total_ref,
    counts_ref, room_ref, mask_ref, counts_sem
):
    span, width = sums_ref.shape
    parts = width // LANES
    each = slots * parts + 1
    me = me_ref[0]
    counts_copy = pltpu.make_async_copy(held_ref, counts_ref, counts_sem)
    counts_copy.start()
    room_ref[...] = jnp.zeros_like(room_ref)
    window = room_ref.shape[0] - span
    spot = lax.broadcasted_iota(jnp.int32, (1, span), 1)
    line = lax.broadcasted_iota(jnp.int32, (window, width), 0)
    padding = jnp.zeros((window - slots, width), jnp.float32)
    counts_copy.wait()
    offset = jnp.int32(0)
    end = jnp.int32(0)
    level = jnp.zeros((1, span), jnp.int32)
    for sender in range(devices):
        base = end
        offset = offset + counts_ref[sender, 0]
        end = lax.div(offset - me + (devices - 1), devices)
        first = sender * each
        chunk = jnp.concatenate(
            [got_ref[first + part * slots : first + (part + 1) * slots, :] for part in range(parts)], axis=1
        )
        shift = base % 8
        chunk = pltpu.roll(jnp.concatenate([chunk, padding], axis=0), shift, 0)
        there = pl.ds(pl.multiple_of(base - shift, 8), window)
        room_ref[there, :] = jnp.where((line >= shift) & (line < shift + end - base), chunk, room_ref[there, :])
        inside = (spot >= base) & (spot < end)
        mask_ref[sender : sender + 1, :] = inside.astype(jnp.float32)
        level = jnp.where(inside, spot - base, level)
    sums_ref[...] = room_ref[:span, :]
    total_ref[0] = offset
    fields = jnp.concatenate(
        [got_ref[(sender + 1) * each - 1 : (sender + 1) * each, :] for sender in range(devices)], axis=0
    )
    picked = lax.dot_general(
        fields,
        mask_ref[...],
        (((0,), (0,)), ((), ())),
        precision=lax.Precision.HIGHEST,
        preferred_element_type=jnp.float32,
    )
    field = lax.broadcasted_iota(jnp.int32, (LANES, span), 0)
    rows = jnp.sum(jnp.where(field == level, picked, 0.0), axis=0, keepdims=True)
    keys = jnp.sum(jnp.where(field == level + slots, picked, 0.0), axis=0, keepdims=True)
    live = spot < end
    rows = jnp.where(live, rows, 0.0).astype(jnp.int32)
    keys = jnp.where(live, keys, -1.0).astype(jnp.int32)
    for part in range(span // LANES):
        rows_ref[part : part + 1, :] = rows[:, part * LANES : (part + 1) * LANES]
        keys_ref[part : part + 1, :] = keys[:, part * LANES : (part + 1) * LANES]


def shards(measures, group_index, distinct_keys, group_counts):
    rows, width = measures.shape
    span = distinct_keys.shape[1]
    devices = lax.axis_size(AXES)
    slots = span // devices
    parts = width // LANES
    each = slots * parts + 1
    me = lax.axis_index(AXES)
    spread = pl.pallas_call(
        spread_kernel,
        in_specs=[pl.BlockSpec(memory_space=pltpu.SMEM)],
        out_specs=pl.BlockSpec(memory_space=pltpu.VMEM),
        out_shape=jax.ShapeDtypeStruct((devices, LANES), jnp.int32),
        compiler_params=pltpu.CompilerParams(vmem_limit_bytes=MIB),
        name="spread",
    )(group_counts)
    counts = lax.all_to_all(spread.reshape(devices, 1, LANES), AXES, split_axis=0, concat_axis=0, tiled=True)
    counts = counts.reshape(devices, LANES)
    packed = pl.pallas_call(
        functools.partial(local_kernel, devices, slots, min(512, rows)),
        in_specs=[pl.BlockSpec(memory_space=pltpu.VMEM)] * 3,
        out_specs=pl.BlockSpec(memory_space=pltpu.VMEM),
        out_shape=jax.ShapeDtypeStruct((2 * devices * each, LANES), jnp.float32),
        scratch_shapes=[pltpu.VMEM((span, width), jnp.float32), pltpu.VMEM((devices, LANES), jnp.float32)],
        cost_estimate=pl.CostEstimate(flops=6 * span * rows * width, bytes_accessed=4 * rows * width, transcendentals=0),
        compiler_params=pltpu.CompilerParams(vmem_limit_bytes=16 * MIB),
        name="local",
    )(group_index.reshape(1, rows), measures, distinct_keys)
    outgoing = pl.pallas_call(
        functools.partial(roll_kernel, devices),
        in_specs=[
            pl.BlockSpec(memory_space=pltpu.SMEM),
            pl.BlockSpec(memory_space=pltpu.VMEM),
            pl.BlockSpec(memory_space=pltpu.VMEM),
        ],
        out_specs=pl.BlockSpec(memory_space=pltpu.HBM),
        out_shape=jax.ShapeDtypeStruct((devices, 1, each * LANES), jnp.float32),
        scratch_shapes=[pltpu.SemaphoreType.DMA],
        compiler_params=pltpu.CompilerParams(vmem_limit_bytes=4 * MIB),
        name="roll",
    )(me.reshape(1), counts, packed.reshape(2 * devices, 1, each * LANES))
    got = lax.all_to_all(outgoing, AXES, split_axis=0, concat_axis=0, tiled=True)
    group_sums, group_rows, group_keys, group_total = pl.pallas_call(
        functools.partial(place_kernel, devices, slots),
        in_specs=[
            pl.BlockSpec(memory_space=pltpu.SMEM),
            pl.BlockSpec(memory_space=pltpu.VMEM),
            pl.BlockSpec(memory_space=pltpu.VMEM),
        ],
        out_specs=[pl.BlockSpec(memory_space=pltpu.VMEM)] * 3 + [pl.BlockSpec(memory_space=pltpu.SMEM)],
        out_shape=[
            jax.ShapeDtypeStruct((span, width), jnp.float32),
            jax.ShapeDtypeStruct((span // LANES, LANES), jnp.int32),
            jax.ShapeDtypeStruct((span // LANES, LANES), jnp.int32),
            jax.ShapeDtypeStruct((1,), jnp.int32),
        ],
        scratch_shapes=[
            pltpu.SMEM((devices, LANES), jnp.int32),
            pltpu.VMEM((span + -(-slots // 8) * 8 + 8, width), jnp.float32),
            pltpu.VMEM((devices, span), jnp.float32),
            pltpu.SemaphoreType.DMA,
        ],
        compiler_params=pltpu.CompilerParams(vmem_limit_bytes=8 * MIB),
        name="place",
    )(me.reshape(1), counts, got.reshape(devices * each, LANES))
    return group_sums, group_rows.reshape(span), group_keys.reshape(span), group_total.reshape(())


def solution(mesh):
    return jax.shard_map(
        shards,
        mesh=mesh,
        in_specs=(P(AXES, None), P(AXES), P(AXES, None), P(AXES)),
        out_specs=(P(AXES, None), P(AXES), P(AXES), P()),
        check_vma=False,
    )
```

```python
import functools

import jax
import jax.numpy as jnp
from jax import lax
from jax.experimental import pallas as pl
from jax.experimental.pallas import tpu as pltpu
from jax.sharding import PartitionSpec as P

AXES = ("gx", "gy", "gz")
LANES = 128
MIB = 1024 * 1024


def split3(x):
    high = x.astype(jnp.bfloat16)
    rest = x - high.astype(jnp.float32)
    middle = rest.astype(jnp.bfloat16)
    low = (rest - middle.astype(jnp.float32)).astype(jnp.bfloat16)
    return high, middle, low


def local_kernel(
    devices, slots, block, all_index_ref, all_values_ref, all_keys_ref, packed_ref,
    index_ref, values_ref, keys_ref, sums_ref, fields_ref, index_sem, keys_sem, sem
):
    index_copy = pltpu.make_async_copy(all_index_ref, index_ref, index_sem)
    keys_copy = pltpu.make_async_copy(all_keys_ref, keys_ref, keys_sem)
    copies = [
        pltpu.make_async_copy(all_values_ref.at[pl.ds(start, block)], values_ref.at[pl.ds(start, block)], sem.at[step])
        for step, start in enumerate(range(0, values_ref.shape[0], block))
    ]
    for copy in [keys_copy, index_copy] + copies:
        copy.start()
    span, width = sums_ref.shape
    rows = values_ref.shape[0]
    parts = width // LANES
    each = slots * parts + 1

    def one_hot(height, place):
        return place == lax.broadcasted_iota(jnp.int32, (height, place.shape[1]), 0)

    def across(left, right):
        return lax.dot_general(left, right, (((1,), (1,)), ((), ())), preferred_element_type=jnp.float32)

    group = lax.broadcasted_iota(jnp.int32, (1, span), 1)
    keys_copy.wait()
    to_residue = one_hot(devices, group % devices).astype(jnp.bfloat16)
    to_level = jnp.where(one_hot(LANES, group // devices + slots), keys_ref[...].astype(jnp.float32), 0.0)
    fields = jnp.zeros(fields_ref.shape, jnp.float32)
    for part in split3(to_level):
        fields = fields + across(to_residue, part)
    index_copy.wait()
    for step, start in enumerate(range(0, rows, block)):
        index = index_ref[:, start : start + block]
        residue = index % devices
        level = index // devices
        hits = one_hot(span, residue * slots + level).astype(jnp.bfloat16)
        copies[step].wait()
        high, middle, low = split3(values_ref[start : start + block, :])
        total = jnp.dot(hits, high, preferred_element_type=jnp.float32)
        total = total + jnp.dot(hits, middle, preferred_element_type=jnp.float32)
        total = total + jnp.dot(hits, low, preferred_element_type=jnp.float32)
        sums_ref[...] = total if start == 0 else sums_ref[...] + total
        fields = fields + across(
            one_hot(devices, residue).astype(jnp.bfloat16), one_hot(LANES, level).astype(jnp.bfloat16)
        )
    fields_ref[...] = fields
    for device in range(devices):
        for copy in (device, device + devices):
            start = copy * each
            for part in range(parts):
                packed_ref[start + part * slots : start + (part + 1) * slots, :] = sums_ref[
                    device * slots : (device + 1) * slots, part * LANES : (part + 1) * LANES
                ]
            packed_ref[start + each - 1 : start + each, :] = fields_ref[device : device + 1, :]


def spread_kernel(count_ref, out_ref):
    out_ref[...] = jnp.full(out_ref.shape, count_ref[0], jnp.int32)


def roll_kernel(devices, me_ref, counts_ref, packed_ref, out_ref, sem):
    counts = counts_ref[...].astype(jnp.float32)
    sender = lax.broadcasted_iota(jnp.int32, counts.shape, 0)
    lane = lax.broadcasted_iota(jnp.int32, counts.shape, 1)
    offset = jnp.sum(jnp.where((sender < me_ref[0]) & (lane == 0), counts, 0.0)).astype(jnp.int32)
    start = devices - lax.rem(offset, devices)
    copy = pltpu.make_async_copy(packed_ref.at[pl.ds(start, devices)], out_ref, sem)
    copy.start()
    copy.wait()


def place_kernel(
    devices, slots, me_ref, held_ref, got_ref, sums_ref, rows_ref, keys_ref, total_ref,
    counts_ref, room_ref, mask_ref, counts_sem
):
    span, width = sums_ref.shape
    parts = width // LANES
    each = slots * parts + 1
    me = me_ref[0]
    counts_copy = pltpu.make_async_copy(held_ref, counts_ref, counts_sem)
    counts_copy.start()
    room_ref[...] = jnp.zeros_like(room_ref)
    window = room_ref.shape[0] - span
    spot = lax.broadcasted_iota(jnp.int32, (1, span), 1)
    line = lax.broadcasted_iota(jnp.int32, (window, width), 0)
    padding = jnp.zeros((window - slots, width), jnp.float32)
    counts_copy.wait()
    offset = jnp.int32(0)
    end = jnp.int32(0)
    level = jnp.zeros((1, span), jnp.int32)
    for sender in range(devices):
        base = end
        offset = offset + counts_ref[sender, 0]
        end = lax.div(offset - me + (devices - 1), devices)
        first = sender * each
        chunk = jnp.concatenate(
            [got_ref[first + part * slots : first + (part + 1) * slots, :] for part in range(parts)], axis=1
        )
        shift = base % 8
        chunk = pltpu.roll(jnp.concatenate([chunk, padding], axis=0), shift, 0)
        there = pl.ds(pl.multiple_of(base - shift, 8), window)
        room_ref[there, :] = jnp.where((line >= shift) & (line < shift + end - base), chunk, room_ref[there, :])
        inside = (spot >= base) & (spot < end)
        mask_ref[sender : sender + 1, :] = inside.astype(jnp.float32)
        level = jnp.where(inside, spot - base, level)
    sums_ref[...] = room_ref[:span, :]
    total_ref[0] = offset
    fields = jnp.concatenate(
        [got_ref[(sender + 1) * each - 1 : (sender + 1) * each, :] for sender in range(devices)], axis=0
    )
    picked = lax.dot_general(
        fields,
        mask_ref[...],
        (((0,), (0,)), ((), ())),
        precision=lax.Precision.HIGHEST,
        preferred_element_type=jnp.float32,
    )
    field = lax.broadcasted_iota(jnp.int32, (LANES, span), 0)
    rows = jnp.sum(jnp.where(field == level, picked, 0.0), axis=0, keepdims=True)
    keys = jnp.sum(jnp.where(field == level + slots, picked, 0.0), axis=0, keepdims=True)
    live = spot < end
    rows = jnp.where(live, rows, 0.0).astype(jnp.int32)
    keys = jnp.where(live, keys, -1.0).astype(jnp.int32)
    for part in range(span // LANES):
        rows_ref[part : part + 1, :] = rows[:, part * LANES : (part + 1) * LANES]
        keys_ref[part : part + 1, :] = keys[:, part * LANES : (part + 1) * LANES]


def shards(measures, group_index, distinct_keys, group_counts):
    rows, width = measures.shape
    span = distinct_keys.shape[1]
    devices = lax.axis_size(AXES)
    slots = span // devices
    parts = width // LANES
    each = slots * parts + 1
    me = lax.axis_index(AXES)
    spread = pl.pallas_call(
        spread_kernel,
        in_specs=[pl.BlockSpec(memory_space=pltpu.SMEM)],
        out_specs=pl.BlockSpec(memory_space=pltpu.VMEM),
        out_shape=jax.ShapeDtypeStruct((devices, LANES), jnp.int32),
        compiler_params=pltpu.CompilerParams(vmem_limit_bytes=MIB),
        name="spread",
    )(group_counts)
    counts = lax.all_to_all(spread.reshape(devices, 1, LANES), AXES, split_axis=0, concat_axis=0, tiled=True)
    counts = counts.reshape(devices, LANES)
    block = min(512, rows)
    packed = pl.pallas_call(
        functools.partial(local_kernel, devices, slots, block),
        in_specs=[pl.BlockSpec(memory_space=pl.ANY)] * 3,
        out_specs=pl.BlockSpec(memory_space=pltpu.VMEM),
        out_shape=jax.ShapeDtypeStruct((2 * devices * each, LANES), jnp.float32),
        scratch_shapes=[
            pltpu.VMEM((1, rows), jnp.int32),
            pltpu.VMEM((rows, width), jnp.float32),
            pltpu.VMEM((1, span), jnp.int32),
            pltpu.VMEM((span, width), jnp.float32),
            pltpu.VMEM((devices, LANES), jnp.float32),
            pltpu.SemaphoreType.DMA,
            pltpu.SemaphoreType.DMA,
            pltpu.SemaphoreType.DMA((rows // block,)),
        ],
        cost_estimate=pl.CostEstimate(flops=6 * span * rows * width, bytes_accessed=4 * rows * width, transcendentals=0),
        compiler_params=pltpu.CompilerParams(vmem_limit_bytes=52 * MIB),
        name="local",
    )(group_index.reshape(1, rows), measures, distinct_keys)
    outgoing = pl.pallas_call(
        functools.partial(roll_kernel, devices),
        in_specs=[
            pl.BlockSpec(memory_space=pltpu.SMEM),
            pl.BlockSpec(memory_space=pltpu.VMEM),
            pl.BlockSpec(memory_space=pltpu.VMEM),
        ],
        out_specs=pl.BlockSpec(memory_space=pl.ANY),
        out_shape=jax.ShapeDtypeStruct((devices, 1, each * LANES), jnp.float32),
        scratch_shapes=[pltpu.SemaphoreType.DMA],
        compiler_params=pltpu.CompilerParams(vmem_limit_bytes=4 * MIB),
        name="roll",
    )(me.reshape(1), counts, packed.reshape(2 * devices, 1, each * LANES))
    got = lax.all_to_all(outgoing, AXES, split_axis=0, concat_axis=0, tiled=True)
    group_sums, group_rows, group_keys, group_total = pl.pallas_call(
        functools.partial(place_kernel, devices, slots),
        in_specs=[
            pl.BlockSpec(memory_space=pltpu.SMEM),
            pl.BlockSpec(memory_space=pltpu.VMEM),
            pl.BlockSpec(memory_space=pltpu.VMEM),
        ],
        out_specs=[pl.BlockSpec(memory_space=pltpu.VMEM)] * 3 + [pl.BlockSpec(memory_space=pltpu.SMEM)],
        out_shape=[
            jax.ShapeDtypeStruct((span, width), jnp.float32),
            jax.ShapeDtypeStruct((span // LANES, LANES), jnp.int32),
            jax.ShapeDtypeStruct((span // LANES, LANES), jnp.int32),
            jax.ShapeDtypeStruct((1,), jnp.int32),
        ],
        scratch_shapes=[
            pltpu.SMEM((devices, LANES), jnp.int32),
            pltpu.VMEM((span + -(-slots // 8) * 8 + 8, width), jnp.float32),
            pltpu.VMEM((devices, span), jnp.float32),
            pltpu.SemaphoreType.DMA,
        ],
        compiler_params=pltpu.CompilerParams(vmem_limit_bytes=8 * MIB),
        name="place",
    )(me.reshape(1), counts, got.reshape(devices * each, LANES))
    return group_sums, group_rows.reshape(span), group_keys.reshape(span), group_total.reshape(())


def solution(mesh):
    return jax.shard_map(
        shards,
        mesh=mesh,
        in_specs=(P(AXES, None), P(AXES), P(AXES, None), P(AXES)),
        out_specs=(P(AXES, None), P(AXES), P(AXES), P()),
        check_vma=False,
    )
```
